32 devices in a mesh: rep: 4 (over x, y), dp: 8 (over z, core).
Axes of the slice: x: 2, y: 2, z: 4, core: 2. Of those that a mesh axis runs over, the one named last changes fastest.
Arguments:
- a: bfloat16 [32, 4, 8192, 1024], P(('rep', 'dp')), parts along dimension 0
- g: bfloat16 [32, 4, 8192, 2560], P(('rep', 'dp')), parts along dimension 0
Outputs:
- output: bfloat16 [16, 1024, 2560], P('rep'), parts along dimension 0
There are 4 independent parts. The reference program is written for one: setup_inputs(seed, part) draws one part's arguments, and reference() takes and returns one part's arrays. A program takes and returns all parts, laid end to end along the dimension named above; each array names one.
All inputs are finite; a program needn't handle non-finite values.
Results may differ from the reference program's by a relative error of at most 0.012.
Values are sent between devices in bfloat16 or wider.
A program may use at most 2 GiB of HBM per device.

```python
import jax
import jax.numpy as jnp
from jax import lax

DEVICES = 8
MATRICES = 4
TOKENS = 8192
D = 1024
FF = 2560


def setup_inputs(seed: int = 0, part: int = 0) -> dict:
    ka, kg, ks = (jax.random.fold_in(k, part) for k in jax.random.split(jax.random.key(seed), 3))
    size = 2.0 ** jax.random.uniform(ks, (DEVICES, MATRICES, 1, 1), jnp.float32, -1.0, 1.0)
    a = jax.random.normal(ka, (DEVICES, MATRICES, TOKENS, D), jnp.float32)
    g = size * jax.random.normal(kg, (DEVICES, MATRICES, TOKENS, FF), jnp.float32) * (DEVICES * TOKENS) ** -0.5
    return {"a": a.astype(jnp.bfloat16), "g": g.astype(jnp.bfloat16)}


def reference(a, g):
    def take(so_far, one):
        return so_far + jnp.einsum("ntd,ntf->ndf", *one, preferred_element_type=jnp.float32), None

    return lax.scan(take, jnp.zeros((MATRICES, D, FF), jnp.float32), (a, g))[0].astype(jnp.bfloat16)
```

```python
import functools

import jax
import jax.numpy as jnp
from jax import lax
from jax.experimental import pallas as pl
from jax.experimental.pallas import tpu as pltpu
from jax.sharding import PartitionSpec as P

MESH = pl.DeviceIdType.MESH
TM, TN = 512, 256
HALF = TM // 2
N_ACC = 6
N_PAIR = 8
N_IN = 16
N_OUT = 8
N_MID = 8
LAG_END, LAG_ADD, LAG_FIN, LAG_FWD = 1, 3, 5, 12


def kernel(shape, a_hbm, g_hbm, out, a_buf, g_buf, acc, pair_out, pair_in, line_out, line_in, mid_in,
           a_sem, g_sem, pair_ssem, pair_rsem, out_ssem, line_rsem, mid_rsem, fin_ssem, fin_rsem, fwd_ssem, fwd_rsem):
    matrices, depth, rows, cols = shape
    per_phase = cols // TN
    phases = matrices * (rows // TM)
    tiles = phases * per_phase
    blocks = rows // TM

    rep, dp = lax.axis_index("rep"), lax.axis_index("dp")
    z, core = dp // 2, dp % 2
    is_end = jnp.logical_or(z == 0, z == 3)
    is_mid = jnp.logical_not(is_end)
    partner = (rep, z * 2 + (1 - core))
    inward = (rep, jnp.where(z < 2, z + 1, z - 1) * 2 + core)
    outward = (rep, jnp.where(z < 2, 0, 3) * 2 + core)
    mine, theirs = core * HALF, (1 - core) * HALF

    def region(ref, t, offset):
        phase = t // per_phase
        row = pl.multiple_of((phase % blocks) * TM + offset, HALF)
        col = pl.multiple_of((t % per_phase) * TN, TN)
        return ref.at[phase // blocks, pl.ds(row, HALF), pl.ds(col, TN)]

    def load_a(p):
        block = pl.multiple_of((p % blocks) * TM, TM)
        return pltpu.make_async_copy(a_hbm.at[p // blocks, :, pl.ds(block, TM)], a_buf.at[p % 2], a_sem.at[p % 2])

    def load_g(t):
        col = pl.multiple_of((t % per_phase) * TN, TN)
        return pltpu.make_async_copy(
            g_hbm.at[t // (per_phase * blocks), :, pl.ds(col, TN)], g_buf.at[t % 2], g_sem.at[t % 2])

    def send(src, dst, ssem, rsem, device):
        return pltpu.make_async_remote_copy(src, dst, ssem, rsem, device_id=device, device_id_type=MESH)

    def pair_copy(t):
        s = t % N_PAIR
        return send(pair_out.at[s], pair_in.at[s], pair_ssem.at[s], pair_rsem.at[s], partner)

    def line_copy(t):
        s, d = t % N_OUT, t % N_IN
        return send(line_out.at[s], line_in.at[d], out_ssem.at[s], line_rsem.at[d], inward)

    def mid_copy(t):
        s, d = t % N_OUT, t % N_MID
        return send(line_out.at[s], mid_in.at[d], out_ssem.at[s], mid_rsem.at[d], inward)

    def fin_copy(t):
        here = region(out, t, mine)
        return send(here, here, fin_ssem, fin_rsem.at[t % N_IN], outward)

    def fwd_copy(t):
        here = region(out, t, mine)
        return send(here, here, fwd_ssem, fwd_rsem, partner)

    load_a(0).start()
    load_g(0).start()
    load_g(1).start()

    barrier = pltpu.get_barrier_semaphore()
    pl.semaphore_signal(barrier, inc=1, device_id=partner, device_id_type=MESH)
    pl.semaphore_signal(barrier, inc=1, device_id=inward, device_id_type=MESH)

    @pl.when(is_mid)
    def _():
        pl.semaphore_signal(barrier, inc=1, device_id=outward, device_id_type=MESH)

    pl.semaphore_wait(barrier, jnp.where(is_mid, 3, 2))

    def compute(t):
        p = t // per_phase

        @pl.when(t % per_phase == 0)
        def _():
            load_a(p).wait()

        load_g(t).wait()
        acc[t % N_ACC] = lax.dot_general(
            a_buf[p % 2], g_buf[t % 2], (((0,), (0,)), ((), ())), preferred_element_type=jnp.float32)

        @pl.when(t + 2 < tiles)
        def _():
            load_g(t + 2).start()

        @pl.when(jnp.logical_and(t % per_phase == 0, p + 1 < phases))
        def _():
            load_a(p + 1).start()

        @pl.when(t >= N_PAIR)
        def _():
            pair_copy(t - N_PAIR).wait_send()

        pair_out[t % N_PAIR] = acc[t % N_ACC, pl.ds(pl.multiple_of(theirs, HALF), HALF)].astype(jnp.bfloat16)
        pair_copy(t).start()

    def chip_sum(t):
        pair_copy(t).wait_recv()
        own = acc[t % N_ACC, pl.ds(pl.multiple_of(mine, HALF), HALF)]
        return own + pair_in[t % N_PAIR].astype(jnp.float32)

    def end_send(t):
        @pl.when(t >= N_OUT)
        def _():
            line_copy(t - N_OUT).wait_send()

        line_out[t % N_OUT] = chip_sum(t).astype(jnp.bfloat16)
        line_copy(t).start()

    def mid_add(t):
        @pl.when(t >= N_OUT)
        def _():
            mid_copy(t - N_OUT).wait_send()

        line_copy(t).wait_recv()
        total = chip_sum(t) + line_in[t % N_IN].astype(jnp.float32)
        line_out[t % N_OUT] = total.astype(jnp.bfloat16)
        mid_copy(t).start()

    def mid_finish(t):
        mid_copy(t).wait_recv()
        total = line_out[t % N_OUT].astype(jnp.float32) + mid_in[t % N_MID].astype(jnp.float32)
        region(out, t, mine)[...] = total.astype(jnp.bfloat16)
        fin_copy(t).start()
        fwd_copy(t).start()

    def end_forward(t):
        fin_copy(t).wait_recv()
        fwd_copy(t).start()

    def between(t, lag, what):
        @pl.when(jnp.logical_and(t >= lag, t < tiles + lag))
        def _():
            what(t - lag)

    def step(t, carry):
        @pl.when(t < tiles)
        def _():
            compute(t)

        @pl.when(is_end)
        def _():
            between(t, LAG_FWD, end_forward)
            between(t, LAG_END, end_send)

        @pl.when(is_mid)
        def _():
            between(t, LAG_ADD, mid_add)
            between(t, LAG_FIN, mid_finish)

        return carry

    lax.fori_loop(0, tiles + LAG_FWD, step, 0)

    for t in range(tiles - N_PAIR, tiles):
        pair_copy(t).wait_send()
    for t in range(tiles - N_OUT, tiles):
        line_copy(t).wait_send()
    half = out.at[pl.ds(0, matrices // 2)]
    whole = send(half, half, fwd_ssem, fwd_rsem, partner)
    whole.wait_send()
    whole.wait_recv()

    @pl.when(is_mid)
    def _():
        send(half, half, fin_ssem, fwd_rsem, outward).wait_send()


def solution(mesh):
    def step(a, g):
        _, matrices, depth, rows = a.shape
        cols = g.shape[-1]
        bf16, f32 = jnp.bfloat16, jnp.float32
        return pl.pallas_call(
            functools.partial(kernel, (matrices, depth, rows, cols)),
            out_shape=pltpu.VMEM((matrices, rows, cols), bf16),
            in_specs=[pl.BlockSpec(memory_space=pltpu.HBM)] * 2,
            out_specs=pl.BlockSpec(memory_space=pltpu.VMEM),
            scratch_shapes=[
                pltpu.VMEM((2, depth, TM), bf16),
                pltpu.VMEM((2, depth, TN), bf16),
                pltpu.VMEM((N_ACC, TM, TN), f32),
                pltpu.VMEM((N_PAIR, HALF, TN), bf16),
                pltpu.VMEM((N_PAIR, HALF, TN), bf16),
                pltpu.VMEM((N_OUT, HALF, TN), bf16),
                pltpu.VMEM((N_IN, HALF, TN), bf16),
                pltpu.VMEM((N_MID, HALF, TN), bf16),
                pltpu.SemaphoreType.DMA((2,)),
                pltpu.SemaphoreType.DMA((2,)),
                pltpu.SemaphoreType.DMA((N_PAIR,)),
                pltpu.SemaphoreType.DMA((N_PAIR,)),
                pltpu.SemaphoreType.DMA((N_OUT,)),
                pltpu.SemaphoreType.DMA((N_IN,)),
                pltpu.SemaphoreType.DMA((N_MID,)),
                pltpu.SemaphoreType.DMA,
                pltpu.SemaphoreType.DMA((N_IN,)),
                pltpu.SemaphoreType.DMA,
                pltpu.SemaphoreType.DMA,
            ],
            compiler_params=pltpu.CompilerParams(
                collective_id=0, has_side_effects=True, vmem_limit_bytes=42 * 2**20),
        )(a[0], g[0])

    return jax.shard_map(
        step, mesh=mesh, in_specs=(P(("rep", "dp")), P(("rep", "dp"))), out_specs=P("rep"), check_vma=False)
```

```python
import functools

import jax
import jax.numpy as jnp
from jax import lax
from jax.experimental import pallas as pl
from jax.experimental.pallas import tpu as pltpu
from jax.sharding import PartitionSpec as P

MESH = pl.DeviceIdType.MESH
TM = 512
STRIP = 128
N_OWN = 8
N_PAIR = 6
N_IN = 10
N_OUT = 4
N_MID = 6
LAG_END, LAG_ADD, LAG_FIN, LAG_FWD = 0, 2, 4, 9
PIECES = 8
FIRST = 4


def kernel(shape, a_hbm, g_hbm, out, a_buf, g_buf, acc, own, pair_out, pair_in, line_out, line_in, mid_in,
           a_sem, g_sem, first_sem, pair_ssem, pair_rsem, out_ssem, line_rsem, mid_rsem, fin_ssem, fin_rsem, fwd_ssem,
           fwd_rsem):
    matrices, depth, rows, cols = shape
    per_phase = cols // (2 * STRIP)
    blocks = rows // TM
    phases = matrices * blocks
    tiles = phases * per_phase

    rep, dp = lax.axis_index("rep"), lax.axis_index("dp")
    z, core = dp // 2, dp % 2
    is_end = jnp.logical_or(z == 0, z == 3)
    is_mid = jnp.logical_not(is_end)
    partner = (rep, z * 2 + (1 - core))
    inward = (rep, jnp.where(z < 2, z + 1, z - 1) * 2 + core)
    outward = (rep, jnp.where(z < 2, 0, 3) * 2 + core)

    def region(t):
        phase = t // per_phase
        row = pl.multiple_of((phase % blocks) * TM, TM)
        col = pl.multiple_of((t % per_phase) * (2 * STRIP) + core * STRIP, STRIP)
        return out.at[phase // blocks, pl.ds(row, TM), pl.ds(col, STRIP)]

    def held(t):
        last = jnp.logical_and(core == 1, t % per_phase == per_phase - 1)
        return jnp.where(last, N_OWN + (t // per_phase) % 2, t % N_OWN)

    def load_a(p, start=0, size=depth):
        block = pl.multiple_of((p % blocks) * TM, TM)
        return pltpu.make_async_copy(
            a_hbm.at[p // blocks, pl.ds(start, size), pl.ds(block, TM)], a_buf.at[p % 2, pl.ds(start, size)],
            a_sem.at[p % 2])

    def load_g(t, strip, start=0, size=depth, sem=None):
        j = t % per_phase
        col = (jnp.where(jnp.logical_and(core == 1, j == 0), per_phase, j) * 2 - core if strip == 0 else j * 2 + 1 - core)
        return pltpu.make_async_copy(
            g_hbm.at[t // (per_phase * blocks), pl.ds(start, size), pl.ds(pl.multiple_of(col * STRIP, STRIP), STRIP)],
            g_buf.at[t % 2, pl.ds(start, size), pl.ds(strip * STRIP, STRIP)], g_sem.at[t % 2] if sem is None else sem)

    def wait_g(t):
        pltpu.make_async_copy(g_buf.at[t % 2], g_buf.at[t % 2], g_sem.at[t % 2]).wait()

    def load_first(k):
        size = depth // FIRST
        part = pl.ds(k * size, size)
        return (pltpu.make_async_copy(a_hbm.at[0, part, pl.ds(0, TM)], a_buf.at[0, part], first_sem.at[0, k]),
                load_g(0, 0, k * size, size, first_sem.at[1, k]), load_g(0, 1, k * size, size, first_sem.at[2, k]))

    def send(src, dst, ssem, rsem, device):
        return pltpu.make_async_remote_copy(src, dst, ssem, rsem, device_id=device, device_id_type=MESH)

    def pair_copy(t):
        s = t % N_PAIR
        return send(pair_out.at[s], pair_in.at[s], pair_ssem.at[s], pair_rsem.at[s], partner)

    def line_copy(t):
        s, d = t % N_OUT, t % N_IN
        return send(line_out.at[s], line_in.at[d], out_ssem.at[s], line_rsem.at[d], inward)

    def mid_copy(t):
        s, d = t % N_OUT, t % N_MID
        return send(line_out.at[s], mid_in.at[d], out_ssem.at[s], mid_rsem.at[d], inward)

    def fin_copy(t):
        return send(region(t), region(t), fin_ssem, fin_rsem.at[t % N_IN], outward)

    def fwd_copy(t):
        return send(region(t), region(t), fwd_ssem, fwd_rsem, partner)

    barrier = pltpu.get_barrier_semaphore()
    pl.semaphore_signal(barrier, inc=1, device_id=partner, device_id_type=MESH)
    pl.semaphore_signal(barrier, inc=1, device_id=inward, device_id_type=MESH)

    @pl.when(is_mid)
    def _():
        pl.semaphore_signal(barrier, inc=1, device_id=outward, device_id_type=MESH)

    def dot(a, g):
        return lax.dot_general(a, g, (((0,), (0,)), ((), ())), preferred_element_type=jnp.float32)

    def compute_first():
        acc[...] = jnp.zeros_like(acc)

        @pl.loop(0, FIRST)
        def _(k):
            for copy in load_first(k):
                copy.wait()
            part = pl.ds(pl.multiple_of(k * (depth // FIRST), depth // FIRST), depth // FIRST)
            acc[...] += dot(a_buf[0, part], g_buf[0, part])

        pl.semaphore_wait(barrier, jnp.where(is_mid, 3, 2))

    def compute_next(t):
        @pl.when(t % per_phase == 0)
        def _():
            load_a(t // per_phase).wait()

        wait_g(t)
        acc[...] = dot(a_buf[(t // per_phase) % 2], g_buf[t % 2])

    def compute(t):
        p, j = t // per_phase, t % per_phase

        @pl.when(t == 0)
        def _():
            compute_first()

        @pl.when(t > 0)
        def _():
            compute_next(t)

        @pl.when(t + 2 < tiles)
        def _():
            load_g(t + 2, 0).start()
            load_g(t + 2, 1).start()

        @pl.when(jnp.logical_and(jnp.logical_and(j > 0, j <= PIECES), p + 1 < phases))
        def _():
            size = depth // PIECES
            load_a(p + 1, pl.multiple_of((j - 1) * size, size), size).start()

        @pl.when(t >= N_PAIR)
        def _():
            pair_copy(t - N_PAIR).wait_send()

        pair_out[t % N_PAIR] = acc[:, STRIP:].astype(jnp.bfloat16)
        pair_copy(t).start()
        mine = jnp.where(core == 0, t, jnp.where(j == 0, t + per_phase - 1, t - 1))
        own[held(mine)] = acc[:, :STRIP]

    def chip_sum(t):
        pair_copy(t).wait_recv()
        return own[held(t)] + pair_in[t % N_PAIR].astype(jnp.float32)

    def end_send(t):
        @pl.when(t >= N_OUT)
        def _():
            line_copy(t - N_OUT).wait_send()

        line_out[t % N_OUT] = chip_sum(t).astype(jnp.bfloat16)
        line_copy(t).start()

    def mid_add(t):
        @pl.when(t >= N_OUT)
        def _():
            mid_copy(t - N_OUT).wait_send()

        line_copy(t).wait_recv()
        total = chip_sum(t) + line_in[t % N_IN].astype(jnp.float32)
        line_out[t % N_OUT] = total.astype(jnp.bfloat16)
        mid_copy(t).start()

    def mid_finish(t):
        mid_copy(t).wait_recv()
        total = line_out[t % N_OUT].astype(jnp.float32) + mid_in[t % N_MID].astype(jnp.float32)
        region(t)[...] = total.astype(jnp.bfloat16)
        fin_copy(t).start()
        fwd_copy(t).start()

    def end_forward(t):
        fin_copy(t).wait_recv()
        fwd_copy(t).start()

    def between(t, lag, what):
        tile = t - lag

        @pl.when(jnp.logical_and(tile >= 0, tile < tiles))
        def _():
            what(tile)

    def step(t, carry):
        @pl.when(t < tiles)
        def _():
            compute(t)

        @pl.when(is_end)
        def _():
            between(t, LAG_END + core, end_send)
            between(t, LAG_FWD, end_forward)

        @pl.when(is_mid)
        def _():
            between(t, LAG_ADD, mid_add)
            between(t, LAG_FIN, mid_finish)

        return carry

    for k in range(FIRST):
        for copy in load_first(k):
            copy.start()
    load_g(1, 0).start()
    load_g(1, 1).start()
    lax.fori_loop(0, tiles + LAG_FWD, step, 0)

    for t in range(tiles - N_PAIR, tiles):
        pair_copy(t).wait_send()
    for t in range(tiles - N_OUT, tiles):
        line_copy(t).wait_send()
    half = out.at[pl.ds(0, matrices // 2)]
    whole = send(half, half, fwd_ssem, fwd_rsem, partner)
    whole.wait_send()
    whole.wait_recv()

    @pl.when(is_mid)
    def _():
        send(half, half, fin_ssem, fwd_rsem, outward).wait_send()


def write_out(held, out, sem):
    matrices = held.shape[0]
    copies = [pltpu.make_async_copy(held.at[n], out.at[n], sem.at[n]) for n in range(matrices)]
    for copy in copies:
        copy.start()
    for copy in copies:
        copy.wait()


def solution(mesh):
    def step(a, g):
        _, matrices, depth, rows = a.shape
        cols = g.shape[-1]
        bf16, f32 = jnp.bfloat16, jnp.float32
        held = pl.pallas_call(
            functools.partial(kernel, (matrices, depth, rows, cols)),
            out_shape=pltpu.VMEM((matrices, rows, cols), bf16),
            in_specs=[pl.BlockSpec(memory_space=pltpu.HBM)] * 2,
            out_specs=pl.BlockSpec(memory_space=pltpu.VMEM),
            scratch_shapes=[
                pltpu.VMEM((2, depth, TM), bf16),
                pltpu.VMEM((2, depth, 2 * STRIP), bf16),
                pltpu.VMEM((TM, 2 * STRIP), f32),
                pltpu.VMEM((N_OWN + 2, TM, STRIP), f32),
                pltpu.VMEM((N_PAIR, TM, STRIP), bf16),
                pltpu.VMEM((N_PAIR, TM, STRIP), bf16),
                pltpu.VMEM((N_OUT, TM, STRIP), bf16),
                pltpu.VMEM((N_IN, TM, STRIP), bf16),
                pltpu.VMEM((N_MID, TM, STRIP), bf16),
                pltpu.SemaphoreType.DMA((2,)),
                pltpu.SemaphoreType.DMA((2,)),
                pltpu.SemaphoreType.DMA((3, FIRST)),
                pltpu.SemaphoreType.DMA((N_PAIR,)),
                pltpu.SemaphoreType.DMA((N_PAIR,)),
                pltpu.SemaphoreType.DMA((N_OUT,)),
                pltpu.SemaphoreType.DMA((N_IN,)),
                pltpu.SemaphoreType.DMA((N_MID,)),
                pltpu.SemaphoreType.DMA,
                pltpu.SemaphoreType.DMA((N_IN,)),
                pltpu.SemaphoreType.DMA,
                pltpu.SemaphoreType.DMA,
            ],
            compiler_params=pltpu.CompilerParams(
                collective_id=0, has_side_effects=True, vmem_limit_bytes=42 * 2**20),
        )(a[0], g[0])
        return pl.pallas_call(
            write_out,
            out_shape=pltpu.HBM((matrices, rows, cols), bf16),
            in_specs=[pl.BlockSpec(memory_space=pl.ANY)],
            out_specs=pl.BlockSpec(memory_space=pltpu.HBM),
            scratch_shapes=[pltpu.SemaphoreType.DMA((matrices,))],
            compiler_params=pltpu.CompilerParams(vmem_limit_bytes=2**20),
        )(held)

    return jax.shard_map(
        step, mesh=mesh, in_specs=(P(("rep", "dp")), P(("rep", "dp"))), out_specs=P("rep"), check_vma=False)
```

```python
import functools

import jax
import jax.numpy as jnp
from jax import lax
from jax.experimental import pallas as pl
from jax.experimental.pallas import tpu as pltpu
from jax.sharding import PartitionSpec as P

MESH = pl.DeviceIdType.MESH
TM = 512
STRIP = 128
N_OWN = 8
N_PAIR = 6
N_IN = 10
N_OUT = 4
N_MID = 6
LAG_END, LAG_ADD, LAG_FIN, LAG_FWD = 0, 2, 4, 9
PIECES = 8
FIRST = 4
SECOND = 2
LAST = 4


def kernel(shape, a_hbm, g_hbm, out, a_buf, g_buf, g_late, acc, own, pair_out, pair_in, line_out, line_in, mid_in,
           a_sem, g_sem, first_sem, second_sem, late_sem, last_rsem, pair_ssem, pair_rsem, out_ssem, in_rsem, mid_rsem, fin_ssem, fwd_ssem,
           fwd_rsem):
    matrices, depth, rows, cols = shape
    per_phase = cols // (2 * STRIP)
    blocks = rows // TM
    phases = matrices * blocks
    tiles = phases * per_phase

    rep, dp = lax.axis_index("rep"), lax.axis_index("dp")
    z, core = dp // 2, dp % 2
    is_end = jnp.logical_or(z == 0, z == 3)
    is_mid = jnp.logical_not(is_end)
    partner = (rep, z * 2 + (1 - core))
    inward = (rep, jnp.where(z < 2, z + 1, z - 1) * 2 + core)
    outward = (rep, jnp.where(z < 2, 0, 3) * 2 + core)

    def region(t):
        phase = t // per_phase
        row = pl.multiple_of((phase % blocks) * TM, TM)
        col = pl.multiple_of((t % per_phase) * (2 * STRIP) + core * STRIP, STRIP)
        return out.at[phase // blocks, pl.ds(row, TM), pl.ds(col, STRIP)]

    def held(t):
        last = jnp.logical_and(core == 1, t % per_phase == per_phase - 1)
        return jnp.where(last, N_OWN + (t // per_phase) % 2, t % N_OWN)

    def load_a(p, start=0, size=depth):
        block = pl.multiple_of((p % blocks) * TM, TM)
        return pltpu.make_async_copy(
            a_hbm.at[p // blocks, pl.ds(start, size), pl.ds(block, TM)], a_buf.at[p % 2, pl.ds(start, size)],
            a_sem.at[p % 2])

    def load_g(t, strip, start=0, size=depth, sem=None):
        j = t % per_phase
        col = (jnp.where(jnp.logical_and(core == 1, j == 0), per_phase, j) * 2 - core if strip == 0 else j * 2 + 1 - core)
        return pltpu.make_async_copy(
            g_hbm.at[t // (per_phase * blocks), pl.ds(start, size), pl.ds(pl.multiple_of(col * STRIP, STRIP), STRIP)],
            g_buf.at[t % 2, pl.ds(start, size), pl.ds(strip * STRIP, STRIP)], g_sem.at[t % 2] if sem is None else sem)

    def wait_g(t):
        pltpu.make_async_copy(g_buf.at[t % 2], g_buf.at[t % 2], g_sem.at[t % 2]).wait()

    def load_first(k):
        size = depth // FIRST
        part = pl.ds(k * size, size)
        return (pltpu.make_async_copy(a_hbm.at[0, part, pl.ds(0, TM)], a_buf.at[0, part], first_sem.at[0, k]),
                load_g(0, 1, k * size, size, first_sem.at[1, k]))

    late = jnp.logical_and(is_end, core == 1)

    def load_first_own(k):
        size = depth // FIRST
        return load_g(0, 0, k * size, size, first_sem.at[2, k])

    def load_late():
        col = (2 * per_phase - 1) * STRIP
        return pltpu.make_async_copy(g_hbm.at[0, :, pl.ds(col, STRIP)], g_late, late_sem)

    def load_second(k):
        size = depth // SECOND
        return load_g(1, 0, k * size, size, second_sem.at[0, k]), load_g(1, 1, k * size, size, second_sem.at[1, k])

    def send(src, dst, ssem, rsem, device):
        return pltpu.make_async_remote_copy(src, dst, ssem, rsem, device_id=device, device_id_type=MESH)

    def pair_copy(t):
        s = t % N_PAIR
        return send(pair_out.at[s], pair_in.at[s], pair_ssem.at[s], pair_rsem.at[s], partner)

    def line_copy(t):
        s, d = t % N_OUT, t % N_IN
        return send(line_out.at[s], line_in.at[d], out_ssem.at[s], in_rsem.at[d], inward)

    def mid_copy(t):
        s, d = t % N_OUT, t % N_MID
        return send(line_out.at[s], mid_in.at[d], out_ssem.at[s], mid_rsem.at[d], inward)

    def fin_copy(t):
        return send(region(t), region(t), fin_ssem, in_rsem.at[t % N_IN], outward)

    def fwd_copy(t):
        return send(region(t), region(t), fwd_ssem, fwd_rsem, partner)

    piece = TM // LAST

    def last_pieces(src, dst, ssem, rsem, device):
        rows_of = [pl.ds(q * piece, piece) for q in range(LAST)]
        return [send(src.at[r], dst.at[r], ssem, last_rsem.at[q] if rsem is None else rsem, device)
                for q, r in enumerate(rows_of)]

    def last_mid():
        t = tiles - 1
        return last_pieces(line_out.at[t % N_OUT], mid_in.at[t % N_MID], out_ssem.at[t % N_OUT], None, inward)

    def last_fin():
        return last_pieces(region(tiles - 1), region(tiles - 1), fin_ssem, None, outward)

    def last_fwd():
        return last_pieces(region(tiles - 1), region(tiles - 1), fwd_ssem, fwd_rsem, partner)

    barrier = pltpu.get_barrier_semaphore()
    pl.semaphore_signal(barrier, inc=1, device_id=partner, device_id_type=MESH)
    pl.semaphore_signal(barrier, inc=1, device_id=inward, device_id_type=MESH)

    @pl.when(is_mid)
    def _():
        pl.semaphore_signal(barrier, inc=1, device_id=outward, device_id_type=MESH)

    def dot(a, g):
        return lax.dot_general(a, g, (((0,), (0,)), ((), ())), preferred_element_type=jnp.float32)

    def compute_in(pieces, load, slot, own_load=None):
        acc[...] = jnp.zeros_like(acc)

        @pl.loop(0, pieces)
        def _(k):
            for copy in load(k):
                copy.wait()
            if own_load is not None:
                @pl.when(jnp.logical_not(late))
                def _():
                    own_load(k).wait()

            part = pl.ds(pl.multiple_of(k * (depth // pieces), depth // pieces), depth // pieces)
            acc[...] += dot(a_buf[0, part], g_buf[slot, part])

    def compute_next(t):
        @pl.when(t % per_phase == 0)
        def _():
            load_a(t // per_phase).wait()

        wait_g(t)
        acc[...] = dot(a_buf[(t // per_phase) % 2], g_buf[t % 2])

    def compute(t):
        p, j = t // per_phase, t % per_phase

        @pl.when(t == 0)
        def _():
            compute_in(FIRST, load_first, 0, load_first_own)
            pl.semaphore_wait(barrier, jnp.where(is_mid, 3, 2))

        @pl.when(t == 1)
        def _():
            compute_in(SECOND, load_second, 1)

        @pl.when(t > 1)
        def _():
            compute_next(t)

        @pl.when(t + 2 < tiles)
        def _():
            load_g(t + 2, 0).start()
            load_g(t + 2, 1).start()

        @pl.when(jnp.logical_and(jnp.logical_and(j > 0, j <= PIECES), p + 1 < phases))
        def _():
            size = depth // PIECES
            load_a(p + 1, pl.multiple_of((j - 1) * size, size), size).start()

        @pl.when(t >= N_PAIR)
        def _():
            pair_copy(t - N_PAIR).wait_send()

        pair_out[t % N_PAIR] = acc[:, STRIP:].astype(jnp.bfloat16)
        pair_copy(t).start()
        mine = jnp.where(core == 0, t, jnp.where(j == 0, t + per_phase - 1, t - 1))
        own[held(mine)] = acc[:, :STRIP]

    def chip_sum(t):
        pair_copy(t).wait_recv()
        return own[held(t)] + pair_in[t % N_PAIR].astype(jnp.float32)

    def end_send(t):
        @pl.when(t >= N_OUT)
        def _():
            line_copy(t - N_OUT).wait_send()

        line_out[t % N_OUT] = chip_sum(t).astype(jnp.bfloat16)
        line_copy(t).start()

    def mid_add(t):
        @pl.when(t >= N_OUT)
        def _():
            mid_copy(t - N_OUT).wait_send()

        line_copy(t).wait_recv()
        total = chip_sum(t) + line_in[t % N_IN].astype(jnp.float32)
        line_out[t % N_OUT] = total.astype(jnp.bfloat16)

        @pl.when(t < tiles - 1)
        def _():
            mid_copy(t).start()

        @pl.when(t == tiles - 1)
        def _():
            for copy in last_mid():
                copy.start()

    def mid_finish(t):
        @pl.when(t < tiles - 1)
        def _():
            mid_copy(t).wait_recv()
            total = line_out[t % N_OUT].astype(jnp.float32) + mid_in[t % N_MID].astype(jnp.float32)
            region(t)[...] = total.astype(jnp.bfloat16)
            fin_copy(t).start()
            fwd_copy(t).start()

        @pl.when(t == tiles - 1)
        def _():
            for q, (mid, fin, fwd) in enumerate(zip(last_mid(), last_fin(), last_fwd())):
                mid.wait_recv()
                here = pl.ds(q * piece, piece)
                total = (line_out[(tiles - 1) % N_OUT, here].astype(jnp.float32)
                         + mid_in[(tiles - 1) % N_MID, here].astype(jnp.float32))
                region(tiles - 1).at[here][...] = total.astype(jnp.bfloat16)
                fin.start()
                fwd.start()

    def end_forward(t):
        @pl.when(t < tiles - 1)
        def _():
            fin_copy(t).wait_recv()
            fwd_copy(t).start()

        @pl.when(t == tiles - 1)
        def _():
            for fin, fwd in zip(last_fin(), last_fwd()):
                fin.wait_recv()
                fwd.start()

    def between(t, lag, what):
        tile = t - lag

        @pl.when(jnp.logical_and(tile >= 0, tile < tiles))
        def _():
            what(tile)

    def step(t, carry):
        @pl.when(t < tiles)
        def _():
            compute(t)

        @pl.when(is_end)
        def _():
            between(t, LAG_END + core, end_send)
            between(t, LAG_FWD, end_forward)

        @pl.when(jnp.logical_and(late, t == 1))
        def _():
            load_late().start()

        @pl.when(jnp.logical_and(late, t == per_phase - 1))
        def _():
            load_late().wait()
            own[held(per_phase - 1)] = dot(a_buf[0], g_late[...])

        @pl.when(is_mid)
        def _():
            between(t, LAG_ADD, mid_add)
            between(t, LAG_FIN, mid_finish)

        return carry

    for k in range(FIRST):
        for copy in load_first(k):
            copy.start()

        @pl.when(jnp.logical_not(late))
        def _(k=k):
            load_first_own(k).start()

    for k in range(SECOND):
        for copy in load_second(k):
            copy.start()

    @pl.when(late)
    def _():
        g_buf[0, :, :STRIP] = jnp.zeros((depth, STRIP), g_buf.dtype)

    lax.fori_loop(0, tiles + LAG_FWD, step, 0)

    for t in range(tiles - N_PAIR, tiles):
        pair_copy(t).wait_send()
    for t in range(tiles - N_OUT, tiles):
        line_copy(t).wait_send()
    half = out.at[pl.ds(0, matrices // 2)]
    whole = send(half, half, fwd_ssem, fwd_rsem, partner)
    whole.wait_send()
    whole.wait_recv()

    @pl.when(is_mid)
    def _():
        send(half, half, fin_ssem, fwd_rsem, outward).wait_send()


def write_out(held, out, sem):
    matrices = held.shape[0]
    copies = [pltpu.make_async_copy(held.at[n], out.at[n], sem.at[n]) for n in range(matrices)]
    for copy in copies:
        copy.start()
    for copy in copies:
        copy.wait()


def solution(mesh):
    def step(a, g):
        _, matrices, depth, rows = a.shape
        cols = g.shape[-1]
        bf16, f32 = jnp.bfloat16, jnp.float32
        held = pl.pallas_call(
            functools.partial(kernel, (matrices, depth, rows, cols)),
            out_shape=pltpu.VMEM((matrices, rows, cols), bf16),
            in_specs=[pl.BlockSpec(memory_space=pltpu.HBM)] * 2,
            out_specs=pl.BlockSpec(memory_space=pltpu.VMEM),
            scratch_shapes=[
                pltpu.VMEM((2, depth, TM), bf16),
                pltpu.VMEM((2, depth, 2 * STRIP), bf16),
                pltpu.VMEM((depth, STRIP), bf16),
                pltpu.VMEM((TM, 2 * STRIP), f32),
                pltpu.VMEM((N_OWN + 2, TM, STRIP), f32),
                pltpu.VMEM((N_PAIR, TM, STRIP), bf16),
                pltpu.VMEM((N_PAIR, TM, STRIP), bf16),
                pltpu.VMEM((N_OUT, TM, STRIP), bf16),
                pltpu.VMEM((N_IN, TM, STRIP), bf16),
                pltpu.VMEM((N_MID, TM, STRIP), bf16),
                pltpu.SemaphoreType.DMA((2,)),
                pltpu.SemaphoreType.DMA((2,)),
                pltpu.SemaphoreType.DMA((3, FIRST)),
                pltpu.SemaphoreType.DMA((2, SECOND)),
                pltpu.SemaphoreType.DMA,
                pltpu.SemaphoreType.DMA((LAST,)),
                pltpu.SemaphoreType.DMA((N_PAIR,)),
                pltpu.SemaphoreType.DMA((N_PAIR,)),
                pltpu.SemaphoreType.DMA((N_OUT,)),
                pltpu.SemaphoreType.DMA((N_IN,)),
                pltpu.SemaphoreType.DMA((N_MID,)),
                pltpu.SemaphoreType.DMA,
                pltpu.SemaphoreType.DMA,
                pltpu.SemaphoreType.DMA,
            ],
            compiler_params=pltpu.CompilerParams(
                collective_id=0, has_side_effects=True, vmem_limit_bytes=42 * 2**20),
        )(a[0], g[0])
        return pl.pallas_call(
            write_out,
            out_shape=pltpu.HBM((matrices, rows, cols), bf16),
            in_specs=[pl.BlockSpec(memory_space=pl.ANY)],
            out_specs=pl.BlockSpec(memory_space=pltpu.HBM),
            scratch_shapes=[pltpu.SemaphoreType.DMA((matrices,))],
            compiler_params=pltpu.CompilerParams(vmem_limit_bytes=2**20),
        )(held)

    return jax.shard_map(
        step, mesh=mesh, in_specs=(P(("rep", "dp")), P(("rep", "dp"))), out_specs=P("rep"), check_vma=False)
```

```python
import functools

import jax
import jax.numpy as jnp
from jax import lax
from jax.experimental import pallas as pl
from jax.experimental.pallas import tpu as pltpu
from jax.sharding import PartitionSpec as P

MESH = pl.DeviceIdType.MESH
TM = 512
STRIP = 128
N_OWN = 8
N_PAIR = 6
N_IN = 10
N_OUT = 4
N_MID = 6
LAG_END, LAG_ADD, LAG_FIN, LAG_FWD = 0, 2, 4, 9
PIECES = 8
FIRST = 4
SECOND = 2
LAST = 2


def kernel(shape, a_hbm, g_hbm, out, a_buf, g_buf, g_late, acc, own, pair_out, pair_in, line_out, line_in, mid_in,
           a_sem, g_sem, first_sem, second_sem, late_sem, last_rsem, pair_ssem, pair_rsem, out_ssem, in_rsem, mid_rsem, fin_ssem, fwd_ssem,
           fwd_rsem):
    matrices, depth, rows, cols = shape
    per_phase = cols // (2 * STRIP)
    blocks = rows // TM
    phases = matrices * blocks
    tiles = phases * per_phase

    rep, dp = lax.axis_index("rep"), lax.axis_index("dp")
    z, core = dp // 2, dp % 2
    is_end = jnp.logical_or(z == 0, z == 3)
    is_mid = jnp.logical_not(is_end)
    partner = (rep, z * 2 + (1 - core))
    inward = (rep, jnp.where(z < 2, z + 1, z - 1) * 2 + core)
    outward = (rep, jnp.where(z < 2, 0, 3) * 2 + core)

    def region(t):
        phase = t // per_phase
        row = pl.multiple_of((phase % blocks) * TM, TM)
        col = pl.multiple_of((t % per_phase) * (2 * STRIP) + core * STRIP, STRIP)
        return out.at[phase // blocks, pl.ds(row, TM), pl.ds(col, STRIP)]

    def held(t):
        last = jnp.logical_and(core == 1, t % per_phase == per_phase - 1)
        return jnp.where(last, N_OWN + (t // per_phase) % 2, t % N_OWN)

    def load_a(p, start=0, size=depth):
        block = pl.multiple_of((p % blocks) * TM, TM)
        return pltpu.make_async_copy(
            a_hbm.at[p // blocks, pl.ds(start, size), pl.ds(block, TM)], a_buf.at[p % 2, pl.ds(start, size)],
            a_sem.at[p % 2])

    def load_g(t, strip, start=0, size=depth, sem=None):
        j = t % per_phase
        col = (jnp.where(jnp.logical_and(core == 1, j == 0), per_phase, j) * 2 - core if strip == 0 else j * 2 + 1 - core)
        return pltpu.make_async_copy(
            g_hbm.at[t // (per_phase * blocks), pl.ds(start, size), pl.ds(pl.multiple_of(col * STRIP, STRIP), STRIP)],
            g_buf.at[t % 2, pl.ds(start, size), pl.ds(strip * STRIP, STRIP)], g_sem.at[t % 2] if sem is None else sem)

    def wait_g(t):
        pltpu.make_async_copy(g_buf.at[t % 2], g_buf.at[t % 2], g_sem.at[t % 2]).wait()

    def load_first(k):
        size = depth // FIRST
        part = pl.ds(k * size, size)
        return (pltpu.make_async_copy(a_hbm.at[0, part, pl.ds(0, TM)], a_buf.at[0, part], first_sem.at[0, k]),
                load_g(0, 1, k * size, size, first_sem.at[1, k]))

    late = jnp.logical_and(is_end, core == 1)

    def load_first_own(k):
        size = depth // FIRST
        return load_g(0, 0, k * size, size, first_sem.at[2, k])

    def load_late():
        col = (2 * per_phase - 1) * STRIP
        return pltpu.make_async_copy(g_hbm.at[0, :, pl.ds(col, STRIP)], g_late, late_sem)

    def load_second(k):
        size = depth // SECOND
        part = pl.ds(k * size, size)
        cols_of = pl.ds(pl.multiple_of((2 - core) * STRIP, STRIP), 2 * STRIP)
        return (pltpu.make_async_copy(g_hbm.at[0, part, cols_of], g_buf.at[1, part], second_sem.at[k]),)

    def send(src, dst, ssem, rsem, device):
        return pltpu.make_async_remote_copy(src, dst, ssem, rsem, device_id=device, device_id_type=MESH)

    def pair_copy(t):
        s = t % N_PAIR
        return send(pair_out.at[s], pair_in.at[s], pair_ssem.at[s], pair_rsem.at[s], partner)

    def line_copy(t):
        s, d = t % N_OUT, t % N_IN
        return send(line_out.at[s], line_in.at[d], out_ssem.at[s], in_rsem.at[d], inward)

    def mid_copy(t):
        s, d = t % N_OUT, t % N_MID
        return send(line_out.at[s], mid_in.at[d], out_ssem.at[s], mid_rsem.at[d], inward)

    def fin_copy(t):
        return send(region(t), region(t), fin_ssem, in_rsem.at[t % N_IN], outward)

    def fwd_copy(t):
        return send(region(t), region(t), fwd_ssem, fwd_rsem, partner)

    piece = TM // LAST

    def last_pieces(src, dst, ssem, rsem, device):
        rows_of = [pl.ds(q * piece, piece) for q in range(LAST)]
        return [send(src.at[r], dst.at[r], ssem, last_rsem.at[q] if rsem is None else rsem, device)
                for q, r in enumerate(rows_of)]

    def last_mid():
        t = tiles - 1
        return last_pieces(line_out.at[t % N_OUT], mid_in.at[t % N_MID], out_ssem.at[t % N_OUT], None, inward)

    def last_fin():
        return last_pieces(region(tiles - 1), region(tiles - 1), fin_ssem, None, outward)

    def last_fwd():
        return last_pieces(region(tiles - 1), region(tiles - 1), fwd_ssem, fwd_rsem, partner)

    barrier = pltpu.get_barrier_semaphore()
    pl.semaphore_signal(barrier, inc=1, device_id=partner, device_id_type=MESH)
    pl.semaphore_signal(barrier, inc=1, device_id=inward, device_id_type=MESH)

    @pl.when(is_mid)
    def _():
        pl.semaphore_signal(barrier, inc=1, device_id=outward, device_id_type=MESH)

    def dot(a, g):
        return lax.dot_general(a, g, (((0,), (0,)), ((), ())), preferred_element_type=jnp.float32)

    def compute_in(pieces, load, slot, own_load=None):
        acc[...] = jnp.zeros_like(acc)

        @pl.loop(0, pieces)
        def _(k):
            for copy in load(k):
                copy.wait()
            if own_load is not None:
                @pl.when(jnp.logical_not(late))
                def _():
                    own_load(k).wait()

            part = pl.ds(pl.multiple_of(k * (depth // pieces), depth // pieces), depth // pieces)
            acc[...] += dot(a_buf[0, part], g_buf[slot, part])

    def compute_next(t):
        @pl.when(t % per_phase == 0)
        def _():
            load_a(t // per_phase).wait()

        wait_g(t)
        acc[...] = dot(a_buf[(t // per_phase) % 2], g_buf[t % 2])

    def compute(t):
        p, j = t // per_phase, t % per_phase

        @pl.when(t == 0)
        def _():
            compute_in(FIRST, load_first, 0, load_first_own)
            pl.semaphore_wait(barrier, jnp.where(is_mid, 3, 2))

        @pl.when(t == 1)
        def _():
            compute_in(SECOND, load_second, 1)

        @pl.when(t > 1)
        def _():
            compute_next(t)

        @pl.when(t + 2 < tiles)
        def _():
            load_g(t + 2, 0).start()
            load_g(t + 2, 1).start()

        @pl.when(jnp.logical_and(jnp.logical_and(j > 0, j <= PIECES), p + 1 < phases))
        def _():
            size = depth // PIECES
            load_a(p + 1, pl.multiple_of((j - 1) * size, size), size).start()

        @pl.when(t >= N_PAIR)
        def _():
            pair_copy(t - N_PAIR).wait_send()

        pair_out[t % N_PAIR] = acc[:, STRIP:].astype(jnp.bfloat16)
        pair_copy(t).start()
        mine = jnp.where(core == 0, t, jnp.where(j == 0, t + per_phase - 1, t - 1))
        own[held(mine)] = acc[:, :STRIP]

    def chip_sum(t):
        pair_copy(t).wait_recv()
        return own[held(t)] + pair_in[t % N_PAIR].astype(jnp.float32)

    def end_send(t):
        @pl.when(t >= N_OUT)
        def _():
            line_copy(t - N_OUT).wait_send()

        line_out[t % N_OUT] = chip_sum(t).astype(jnp.bfloat16)
        line_copy(t).start()

    def mid_add(t):
        @pl.when(t >= N_OUT)
        def _():
            mid_copy(t - N_OUT).wait_send()

        line_copy(t).wait_recv()
        total = chip_sum(t) + line_in[t % N_IN].astype(jnp.float32)
        line_out[t % N_OUT] = total.astype(jnp.bfloat16)

        @pl.when(t < tiles - 1)
        def _():
            mid_copy(t).start()

        @pl.when(t == tiles - 1)
        def _():
            for copy in last_mid():
                copy.start()

    def mid_finish(t):
        @pl.when(t < tiles - 1)
        def _():
            mid_copy(t).wait_recv()
            total = line_out[t % N_OUT].astype(jnp.float32) + mid_in[t % N_MID].astype(jnp.float32)
            region(t)[...] = total.astype(jnp.bfloat16)
            fin_copy(t).start()
            fwd_copy(t).start()

        @pl.when(t == tiles - 1)
        def _():
            for q, (mid, fin, fwd) in enumerate(zip(last_mid(), last_fin(), last_fwd())):
                mid.wait_recv()
                here = pl.ds(q * piece, piece)
                total = (line_out[(tiles - 1) % N_OUT, here].astype(jnp.float32)
                         + mid_in[(tiles - 1) % N_MID, here].astype(jnp.float32))
                region(tiles - 1).at[here][...] = total.astype(jnp.bfloat16)
                fin.start()
                fwd.start()

    def end_forward(t):
        @pl.when(t < tiles - 1)
        def _():
            fin_copy(t).wait_recv()
            fwd_copy(t).start()

        @pl.when(t == tiles - 1)
        def _():
            for fin, fwd in zip(last_fin(), last_fwd()):
                fin.wait_recv()
                fwd.start()

    def between(t, lag, what):
        tile = t - lag

        @pl.when(jnp.logical_and(tile >= 0, tile < tiles))
        def _():
            what(tile)

    def step(t, carry):
        @pl.when(t < tiles)
        def _():
            compute(t)

        @pl.when(is_end)
        def _():
            between(t, LAG_END + core, end_send)
            between(t, LAG_FWD, end_forward)

        @pl.when(jnp.logical_and(late, t == 1))
        def _():
            load_late().start()

        @pl.when(jnp.logical_and(late, t == per_phase - 1))
        def _():
            load_late().wait()
            own[held(per_phase - 1)] = dot(a_buf[0], g_late[...])

        @pl.when(is_mid)
        def _():
            between(t, LAG_ADD, mid_add)
            between(t, LAG_FIN, mid_finish)

        return carry

    for k in range(FIRST):
        for copy in load_first(k):
            copy.start()

        @pl.when(jnp.logical_not(late))
        def _(k=k):
            load_first_own(k).start()

    for k in range(SECOND):
        for copy in load_second(k):
            copy.start()

    @pl.when(late)
    def _():
        g_buf[0, :, :STRIP] = jnp.zeros((depth, STRIP), g_buf.dtype)

    lax.fori_loop(0, tiles + LAG_FWD, step, 0)

    for t in range(tiles - N_PAIR, tiles):
        pair_copy(t).wait_send()
    for t in range(tiles - N_OUT, tiles):
        line_copy(t).wait_send()
    half = out.at[pl.ds(0, matrices // 2)]
    whole = send(half, half, fwd_ssem, fwd_rsem, partner)
    whole.wait_send()
    whole.wait_recv()

    @pl.when(is_mid)
    def _():
        send(half, half, fin_ssem, fwd_rsem, outward).wait_send()


def write_out(held, out, sem):
    matrices = held.shape[0]
    copies = [pltpu.make_async_copy(held.at[n], out.at[n], sem.at[n]) for n in range(matrices)]
    for copy in copies:
        copy.start()
    for copy in copies:
        copy.wait()


def solution(mesh):
    def step(a, g):
        _, matrices, depth, rows = a.shape
        cols = g.shape[-1]
        bf16, f32 = jnp.bfloat16, jnp.float32
        held = pl.pallas_call(
            functools.partial(kernel, (matrices, depth, rows, cols)),
            out_shape=pltpu.VMEM((matrices, rows, cols), bf16),
            in_specs=[pl.BlockSpec(memory_space=pltpu.HBM)] * 2,
            out_specs=pl.BlockSpec(memory_space=pltpu.VMEM),
            scratch_shapes=[
                pltpu.VMEM((2, depth, TM), bf16),
                pltpu.VMEM((2, depth, 2 * STRIP), bf16),
                pltpu.VMEM((depth, STRIP), bf16),
                pltpu.VMEM((TM, 2 * STRIP), f32),
                pltpu.VMEM((N_OWN + 2, TM, STRIP), f32),
                pltpu.VMEM((N_PAIR, TM, STRIP), bf16),
                pltpu.VMEM((N_PAIR, TM, STRIP), bf16),
                pltpu.VMEM((N_OUT, TM, STRIP), bf16),
                pltpu.VMEM((N_IN, TM, STRIP), bf16),
                pltpu.VMEM((N_MID, TM, STRIP), bf16),
                pltpu.SemaphoreType.DMA((2,)),
                pltpu.SemaphoreType.DMA((2,)),
                pltpu.SemaphoreType.DMA((3, FIRST)),
                pltpu.SemaphoreType.DMA((SECOND,)),
                pltpu.SemaphoreType.DMA,
                pltpu.SemaphoreType.DMA((LAST,)),
                pltpu.SemaphoreType.DMA((N_PAIR,)),
                pltpu.SemaphoreType.DMA((N_PAIR,)),
                pltpu.SemaphoreType.DMA((N_OUT,)),
                pltpu.SemaphoreType.DMA((N_IN,)),
                pltpu.SemaphoreType.DMA((N_MID,)),
                pltpu.SemaphoreType.DMA,
                pltpu.SemaphoreType.DMA,
                pltpu.SemaphoreType.DMA,
            ],
            compiler_params=pltpu.CompilerParams(
                collective_id=0, has_side_effects=True, vmem_limit_bytes=42 * 2**20),
        )(a[0], g[0])
        return pl.pallas_call(
            write_out,
            out_shape=pltpu.HBM((matrices, rows, cols), bf16),
            in_specs=[pl.BlockSpec(memory_space=pl.ANY)],
            out_specs=pl.BlockSpec(memory_space=pltpu.HBM),
            scratch_shapes=[pltpu.SemaphoreType.DMA((matrices,))],
            compiler_params=pltpu.CompilerParams(vmem_limit_bytes=2**20),
        )(held)

    return jax.shard_map(
        step, mesh=mesh, in_specs=(P(("rep", "dp")), P(("rep", "dp"))), out_specs=P("rep"), check_vma=False)
```
